16 devices in a mesh: dp: 2 (over y, z), tp: 8 (over x, core).
Axes of the slice: x: 4, y: 2, z: 1, core: 2. Of those that a mesh axis runs over, the one named last changes fastest.
The devices are a block of a 4x4x8 slice.
Arguments:
- x_in: float32 [16, 256, 2304], P('dp', 'tp'), parts along dimension 0
- d_out: bfloat16 [16, 256, 2304], P('dp', 'tp'), parts along dimension 0
- lengths: int32 [16], P('dp'), parts along dimension 0
- w_qkv: bfloat16 [3, 2304, 3, 24, 96], P(None, None, None, 'tp')
- w_out: bfloat16 [3, 24, 96, 2304], P(None, 'tp')
- w_up: bfloat16 [3, 2304, 9216], P(None, None, 'tp')
- b_up: float32 [3, 9216], P(None, 'tp')
- w_down: bfloat16 [3, 9216, 2304], P(None, 'tp')
- vec_par: float32 [3, 6, 2304], replicated
Outputs:
- output 1: float32 [16, 256, 2304], P('dp', 'tp'), parts along dimension 0
- output 2: float32 [16, 256, 2304], P('dp', 'tp'), parts along dimension 0
- output 3: bfloat16 [6, 2304, 3, 24, 96], P('dp', None, None, 'tp'), parts along dimension 0
- output 4: bfloat16 [6, 24, 96, 2304], P('dp', 'tp'), parts along dimension 0
- output 5: bfloat16 [6, 2304, 9216], P('dp', None, 'tp'), parts along dimension 0
- output 6: float32 [6, 9216], P('dp', 'tp'), parts along dimension 0
- output 7: bfloat16 [6, 9216, 2304], P('dp', 'tp'), parts along dimension 0
- output 8: float32 [6, 6, 2304], P('dp'), parts along dimension 0
There are 2 independent parts. The reference program is written for one: setup_inputs(seed, part) draws one part's arguments, and reference() takes and returns one part's arrays. A program takes and returns all parts, laid end to end along the dimension named above; an argument that names none is the same for every part.
All inputs are finite; a program needn't handle non-finite values.
Results may differ from the reference program's by a relative error of at most 0.02.
Values are sent between devices in bfloat16 or wider.
A program may use at most 768 MiB of HBM per device.

```python
import functools
import jax
import jax.numpy as jnp
from jax import lax

BATCH_GROUP = 8
SEQ_LEN = 256
D_MODEL = 2304
NUM_HEADS = 24
HEAD_DIM = 96
FF_DIM = 9216
LAYERS = 3


def draw_lengths(key_len, key_perm):
    lengths = jax.random.randint(key_len, (BATCH_GROUP,), SEQ_LEN // 4, SEQ_LEN + 1, jnp.int32)
    perm_order = jax.random.permutation(key_perm, BATCH_GROUP)
    return lengths.at[perm_order[0]].set(SEQ_LEN).at[perm_order[1]].set(SEQ_LEN // 4)


def setup_inputs(seed: int = 0, part: int = 0) -> dict:
    shared_key = jax.random.key(seed)
    part_key = jax.random.fold_in(jax.random.key(seed + 1), part)
    key_qkv, key_out, key_up, key_bup, key_down, key_vec = jax.random.split(shared_key, 6)
    key_x, key_dy, key_len, key_perm = jax.random.split(part_key, 4)
    inner_dim = NUM_HEADS * HEAD_DIM
    w_qkv = (jax.random.normal(key_qkv, (LAYERS, D_MODEL, 3, NUM_HEADS, HEAD_DIM), jnp.float32) * (1.2 * D_MODEL ** -0.5)).astype(jnp.bfloat16)
    w_out = (jax.random.normal(key_out, (LAYERS, NUM_HEADS, HEAD_DIM, D_MODEL), jnp.float32) * (2.0 * inner_dim ** -0.5)).astype(jnp.bfloat16)
    w_up = (jax.random.normal(key_up, (LAYERS, D_MODEL, FF_DIM), jnp.float32) * D_MODEL ** -0.5).astype(jnp.bfloat16)
    b_up = jax.random.normal(key_bup, (LAYERS, FF_DIM), jnp.float32) * 0.5
    w_down = (jax.random.normal(key_down, (LAYERS, FF_DIM, D_MODEL), jnp.float32) * (2.0 * FF_DIM ** -0.5)).astype(jnp.bfloat16)
    row_scale = jnp.array([0.25, 0.5, 0.25, 0.5, 0.5, 0.5], jnp.float32)[None, :, None]
    row_base = jnp.array([1.0, 0.0, 1.0, 0.0, 0.0, 0.0], jnp.float32)[None, :, None]
    vec_par = jax.random.normal(key_vec, (LAYERS, 6, D_MODEL), jnp.float32) * row_scale + row_base
    x_in = jax.random.normal(key_x, (BATCH_GROUP, SEQ_LEN, D_MODEL), jnp.float32)
    d_out = jax.random.normal(key_dy, (BATCH_GROUP, SEQ_LEN, D_MODEL), jnp.float32).astype(jnp.bfloat16)
    lengths = draw_lengths(key_len, key_perm)
    return {'x_in': x_in, 'd_out': d_out, 'lengths': lengths, 'w_qkv': w_qkv, 'w_out': w_out, 'w_up': w_up, 'b_up': b_up, 'w_down': w_down, 'vec_par': vec_par}


def layer_norm(x_val, gain_vec, shift_vec):
    row_mean = jnp.mean(x_val, axis=-1, keepdims=True)
    centered = x_val - row_mean
    row_var = jnp.mean(centered * centered, axis=-1, keepdims=True)
    return centered * lax.rsqrt(row_var + 1e-5) * gain_vec + shift_vec


def attend_one(item_tuple):
    q_one, k_one, v_one, length = item_tuple
    scores = jnp.einsum('hqe,hke->hqk', q_one.astype(jnp.float32), k_one.astype(jnp.float32)) * HEAD_DIM ** -0.5
    positions = jnp.arange(SEQ_LEN)
    allowed = (positions[None, :] <= positions[:, None]) & (positions[None, :] < length)
    scores = jnp.where(allowed[None], scores, -1e30)
    attn_prob = jax.nn.softmax(scores, axis=-1).astype(jnp.bfloat16)
    context = jnp.einsum('hqk,hke->hqe', attn_prob.astype(jnp.float32), v_one.astype(jnp.float32))
    return context.astype(jnp.bfloat16)


def gpt_layer(x_val, layer_par, lengths):
    w_qkv, w_out, w_up, b_up, w_down, vec_layer = layer_par
    a_in = layer_norm(x_val, vec_layer[0], vec_layer[1]).astype(jnp.bfloat16)
    qkv_all = jnp.einsum('bsd,dthe->tbhse', a_in.astype(jnp.float32), w_qkv.astype(jnp.float32)).astype(jnp.bfloat16)
    context = lax.map(attend_one, (qkv_all[0], qkv_all[1], qkv_all[2], lengths))
    attn_out = jnp.einsum('bhse,hed->bsd', context.astype(jnp.float32), w_out.astype(jnp.float32)).astype(jnp.bfloat16)
    hidden = x_val + attn_out.astype(jnp.float32) + vec_layer[4]
    a_mid = layer_norm(hidden, vec_layer[2], vec_layer[3]).astype(jnp.bfloat16)
    pre_act = jnp.einsum('bsd,df->bsf', a_mid.astype(jnp.float32), w_up.astype(jnp.float32)) + b_up
    act_bf = jax.nn.gelu(pre_act, approximate=True).astype(jnp.bfloat16)
    mlp_out = jnp.einsum('bsf,fd->bsd', act_bf.astype(jnp.float32), w_down.astype(jnp.float32)).astype(jnp.bfloat16)
    return hidden + mlp_out.astype(jnp.float32) + vec_layer[5]


def forward_stack(x_in, w_qkv, w_out, w_up, b_up, w_down, vec_par, lengths):
    def scan_step(carry_x, layer_par):
        return gpt_layer(carry_x, layer_par, lengths), None
    return lax.scan(scan_step, x_in, (w_qkv, w_out, w_up, b_up, w_down, vec_par))[0]


def reference(x_in, d_out, lengths, w_qkv, w_out, w_up, b_up, w_down, vec_par):
    y_out, pullback = jax.vjp(functools.partial(forward_stack, lengths=lengths), x_in, w_qkv, w_out, w_up, b_up, w_down, vec_par)
    grad_list = pullback(d_out.astype(jnp.float32))
    return (y_out, grad_list[0], grad_list[1], grad_list[2], grad_list[3], grad_list[4], grad_list[5], grad_list[6])
```

```python
import functools
import jax
import jax.numpy as jnp
from jax import lax
from jax.experimental import pallas as pl
from jax.experimental.pallas import tpu as pltpu
from jax.sharding import PartitionSpec as P

TENSOR_AXIS = 'tp'
PARTS_AXIS = 'dp'
MESH = pl.DeviceIdType.MESH
F32 = jnp.float32
BF16 = jnp.bfloat16
GROUPS = 2
LANES = 128
N_COPIES = 23
VMEM_LIMIT = 67043328
ANY = pl.BlockSpec(memory_space=pl.ANY)
VMEM = pl.BlockSpec(memory_space=pltpu.VMEM)
SMEM = pl.BlockSpec(memory_space=pltpu.SMEM)


def dot_nn(lhs, rhs):
    return lax.dot_general(lhs, rhs, (((1,), (0,)), ((), ())), preferred_element_type=F32)


def dot_nt(lhs, rhs):
    return lax.dot_general(lhs, rhs, (((1,), (1,)), ((), ())), preferred_element_type=F32)


def dot_tn(lhs, rhs):
    return lax.dot_general(lhs, rhs, (((0,), (0,)), ((), ())), preferred_element_type=F32)


class Ring:
    def __init__(self, n_dev, src, full, pbuf, precv, r_far, r_near, out, send_sem, recv_sem, own_sem):
        self.src, self.full, self.pbuf, self.precv = src, full, pbuf, precv
        self.r_far, self.r_near, self.out = r_far, r_near, out
        self.send_sem, self.recv_sem, self.own_sem = send_sem, recv_sem, own_sem
        self.rows = src.shape[1]
        self.half = self.rows // 2
        n_chips = n_dev // 2
        me = lax.axis_index(TENSOR_AXIS)
        chip, core = me // 2, me % 2
        self.me, self.core = me, core
        self.right_chip, self.left_chip = (chip + 1) % n_chips, (chip + n_chips - 1) % n_chips
        self.far_chip = (chip + 2) % n_chips
        self.chips = (self.far_chip, self.right_chip, self.left_chip, chip)
        self.partner = chip * 2 + 1 - core
        self.right, self.left, self.far = self.right_chip * 2 + core, self.left_chip * 2 + core, self.far_chip * 2 + core
        self.sent = []

    def barrier(self):
        sem = pltpu.get_barrier_semaphore()
        for dev in (self.partner, self.left, self.right):
            pl.semaphore_signal(sem, inc=1, device_id={TENSOR_AXIS: dev}, device_id_type=MESH)
        pl.semaphore_wait(sem, 3)

    def copy(self, grp, idx, src, dst, dev):
        return pltpu.make_async_remote_copy(src_ref=src, dst_ref=dst, send_sem=self.send_sem.at[grp, idx],
                                            recv_sem=self.recv_sem.at[grp, idx], device_id={TENSOR_AXIS: dev}, device_id_type=MESH)

    def start(self, grp, idx, src, dst, dev):
        desc = self.copy(grp, idx, src, dst, dev)
        desc.start()
        self.sent.append(desc)

    def arrive(self, grp, idx, dst, dev):
        self.copy(grp, idx, dst, dst, dev).wait_recv()

    def slot(self, grp, shard, part=None):
        if part is None:
            return self.full.at[grp, pl.ds(pl.multiple_of(shard * self.rows, self.rows), self.rows), :]
        return self.full.at[grp, pl.ds(pl.multiple_of(shard * self.rows + part * self.half, self.half), self.half), :]

    def src_half(self, grp, part):
        return self.src.at[grp, pl.ds(part * self.half, self.half), :]

    def issue_own(self, grp):
        pltpu.make_async_copy(self.src.at[grp], self.slot(grp, self.me), self.own_sem.at[grp]).start()
        self.start(grp, 1, self.src_half(grp, 0), self.slot(grp, self.me, 0), self.right)
        self.start(grp, 3, self.src_half(grp, 1), self.slot(grp, self.me, 1), self.left)
        self.start(grp, 2, self.src_half(grp, 1), self.slot(grp, self.me, 1), self.right)
        self.start(grp, 4, self.src_half(grp, 0), self.slot(grp, self.me, 0), self.left)
        self.start(grp, 0, self.src.at[grp], self.slot(grp, self.me), self.partner)

    def pass_on(self, grp, idx, idx_next, idx_side, shard, part, dev_from, dev_to):
        here = self.slot(grp, shard, part)
        self.arrive(grp, idx, here, dev_from)
        if idx_next is not None:
            self.start(grp, idx_next, here, here, dev_to)
        self.start(grp, idx_side, here, here, self.partner)

    def serve_first(self, grp):
        self.pass_on(grp, 1, 5, 7, self.left, 0, self.left, self.right)
        self.pass_on(grp, 3, 6, 9, self.right, 1, self.right, self.left)

    def serve_second(self, grp):
        self.pass_on(grp, 2, None, 8, self.left, 1, self.left, None)
        self.pass_on(grp, 4, None, 10, self.right, 0, self.right, None)

    def serve_far(self, grp):
        self.pass_on(grp, 5, None, 11, self.far, 0, self.left, None)
        self.pass_on(grp, 6, None, 12, self.far, 1, self.right, None)

    def wait_full(self, grp):
        pltpu.make_async_copy(self.src.at[grp], self.slot(grp, self.me), self.own_sem.at[grp]).wait()
        other = 1 - self.core
        left, right, far = self.left_chip * 2 + other, self.right_chip * 2 + other, self.far_chip * 2 + other
        self.arrive(grp, 0, self.slot(grp, self.partner), self.partner)
        for idx, shard, part in ((7, left, 0), (9, right, 1), (8, left, 1), (10, right, 0), (11, far, 0), (12, far, 1)):
            self.arrive(grp, idx, self.slot(grp, shard, part), self.partner)

    def send_part(self, grp, k):
        self.start(grp, 13 + k, self.pbuf.at[grp, k, 1 - self.core], self.precv.at[grp, k], self.partner)

    def sum_part(self, grp, k):
        mine = self.precv.at[grp, k]
        self.arrive(grp, 13 + k, mine, self.partner)
        total = self.pbuf[grp, k, self.core].astype(F32) + mine[...].astype(F32)
        mine[...] = total.astype(BF16)
        first, second = mine.at[pl.ds(0, self.half), :], mine.at[pl.ds(self.half, self.half), :]
        if k == 0:
            self.start(grp, 17, first, self.r_far.at[grp, 0], self.right)
            self.start(grp, 18, second, self.r_far.at[grp, 1], self.left)
        elif k == 1:
            self.start(grp, 19, second, self.r_near.at[grp, 0, pl.ds(self.half, self.half), :], self.right)
        elif k == 2:
            self.start(grp, 20, first, self.r_near.at[grp, 1, pl.ds(0, self.half), :], self.left)

    def relay(self, grp):
        for k, side, part, idx_in, idx_out, dev_from, dev_to in (
                (1, 0, 0, 17, 21, self.left, self.right), (2, 1, 1, 18, 22, self.right, self.left)):
            landed = self.r_far.at[grp, side]
            self.arrive(grp, idx_in, landed, dev_from)
            part_rows = pl.ds(part * self.half, self.half)
            mine = self.precv.at[grp, k, part_rows, :]
            mine[...] = (mine[...].astype(F32) + landed[...].astype(F32)).astype(BF16)
            self.start(grp, idx_out, mine, self.r_near.at[grp, side, part_rows, :], dev_to)

    def finish(self, grp):
        low, high = pl.ds(0, self.half), pl.ds(self.half, self.half)
        self.arrive(grp, 19, self.r_near.at[grp, 0, high, :], self.left)
        self.arrive(grp, 20, self.r_near.at[grp, 1, low, :], self.right)
        self.arrive(grp, 21, self.r_near.at[grp, 0, low, :], self.left)
        self.arrive(grp, 22, self.r_near.at[grp, 1, high, :], self.right)
        total = self.precv[grp, 3].astype(F32) + self.r_near[grp, 0].astype(F32) + self.r_near[grp, 1].astype(F32)
        self.out[grp] = total.astype(BF16)

    def drain(self):
        for desc in self.sent:
            desc.wait_send()


def run_schedule(ring, stages, part_dot, on_full, head=((), (), ()), tail=((), (), ())):
    def fill(work):
        for fn in work:
            fn()

    def parts(grp, k):
        rows = ring.rows
        row0 = pl.multiple_of(ring.chips[k] * 2 * rows, 2 * rows)
        width = ring.out.shape[2]
        tile = width // 3

        def column(step, carry):
            cols = pl.ds(pl.multiple_of(step * tile, tile), tile)
            val = part_dot(grp, row0, 2 * rows, step * tile, tile).astype(BF16)
            ring.pbuf[grp, k, 0, :, cols] = val[:rows]
            ring.pbuf[grp, k, 1, :, cols] = val[rows:]
            return carry
        lax.fori_loop(0, 3, column, 0)
        ring.send_part(grp, k)

    ring.issue_own(0)
    fill(head[0])
    ring.serve_first(0)
    ring.issue_own(1)
    fill(head[1])
    ring.serve_second(0)
    fill(head[2])
    ring.serve_far(0)
    ring.wait_full(0)
    on_full(0)
    stages_0 = stages(0)
    stages_0[0]()
    ring.serve_first(1)
    for fn in stages_0[1:]:
        fn()
    parts(0, 0)
    ring.serve_second(1)
    parts(0, 1)
    ring.sum_part(0, 0)
    parts(0, 2)
    ring.sum_part(0, 1)
    parts(0, 3)
    ring.sum_part(0, 2)
    ring.serve_far(1)
    ring.sum_part(0, 3)
    ring.wait_full(1)
    on_full(1)
    stages_1 = stages(1)
    stages_1[0]()
    ring.relay(0)
    for fn in stages_1[1:]:
        fn()
    parts(1, 0)
    parts(1, 1)
    ring.sum_part(1, 0)
    parts(1, 2)
    ring.sum_part(1, 1)
    parts(1, 3)
    ring.sum_part(1, 2)
    fill(tail[0])
    ring.finish(0)
    ring.sum_part(1, 3)
    fill(tail[1])
    ring.relay(1)
    fill(tail[2])
    ring.finish(1)
    ring.drain()


def row_blocks(n_rows, block, body):
    def step(i, carry):
        body(pl.multiple_of(i * block, block))
        return carry
    lax.fori_loop(0, n_rows // block, step, 0)


class Stager:
    def __init__(self, buf, sem):
        self.buf, self.sem, self.pending, self.count = buf, sem, [None, None], 0

    def put(self, pieces, view, dst):
        slot = self.count % 2
        self.count += 1
        if self.pending[slot] is not None:
            self.pending[slot].wait()
        start = 0
        for piece in pieces:
            val = piece().astype(self.buf.dtype)
            lanes = pl.ds(start, val.shape[1])
            start += val.shape[1]
            if len(self.buf.shape) == 4:
                self.buf[slot, :, :, lanes] = val.reshape(self.buf.shape[1], self.buf.shape[2], val.shape[1])
            else:
                self.buf[slot, :, lanes] = val
        copy = pltpu.make_async_copy(view(self.buf.at[slot]), dst, self.sem.at[slot])
        copy.start()
        self.pending[slot] = copy

    def drain(self):
        for copy in self.pending:
            if copy is not None:
                copy.wait()


def load_heads(hbm, vmem, sem, pad):
    head_dim = hbm.shape[1]
    copy = pltpu.make_async_copy(hbm, vmem.at[:, pl.ds(0, head_dim), :], sem)
    copy.start()
    if pad:
        vmem[:, head_dim:, :] = jnp.zeros((vmem.shape[0], LANES - head_dim, vmem.shape[2]), vmem.dtype)
    return copy


def softmax_probs(q_val, k_val, length, scale):
    scores = dot_nt(q_val, k_val) * scale
    row = lax.broadcasted_iota(jnp.int32, scores.shape, 0)
    col = lax.broadcasted_iota(jnp.int32, scores.shape, 1)
    scores = jnp.where((col <= row) & (col < length), scores, -1e30)
    expd = jnp.exp(scores - jnp.max(scores, axis=1, keepdims=True))
    return expd / jnp.sum(expd, axis=1, keepdims=True)


def seq_rows(ref, grp, seq, head):
    block = ref[grp, :, seq, :, head * LANES:(head + 1) * LANES]
    return block.reshape(block.shape[0] * block.shape[1], LANES)


def put_seq(ref, grp, seq, head, val):
    n_dev, pos = ref.shape[1], ref.shape[3]
    ref[grp, :, seq, :, head * LANES:(head + 1) * LANES] = val.reshape(n_dev, pos, LANES)


def attn_fwd_kernel(n_dev, n_heads, scale, src, lengths, w_in, w_out, out, full_out, qkv_out, ctx_out,
                    full, qkv, ctx, w_in_v, w_out_v, pbuf, precv, r_far, r_near, send_sem, recv_sem, own_sem, local_sem):
    ring = Ring(n_dev, src, full, pbuf, precv, r_far, r_near, out, send_sem, recv_sem, own_sem)
    ring.barrier()
    load_in = load_heads(w_in, w_in_v, local_sem.at[0], True)
    load_out = load_heads(w_out, w_out_v, local_sem.at[1], True)
    saves = []
    n_seq, pos = qkv.shape[2], qkv.shape[3]
    n_rows, d_model = full.shape[1], full.shape[2]
    shard_rows = n_seq * pos

    def save(src_ref, dst_ref, idx):
        copy = pltpu.make_async_copy(src_ref, dst_ref, local_sem.at[idx])
        copy.start()
        saves.append(copy)

    def on_full(grp):
        if grp == 0:
            load_in.wait()
            load_out.wait()
        save(full.at[grp], full_out.at[grp], 2 + grp)

    def stages(grp):
        def project():
            def body(row0):
                w_all = w_in_v[...].reshape(w_in_v.shape[0] * LANES, d_model)
                val = dot_nt(full[grp, pl.ds(row0, 2 * shard_rows), :], w_all).astype(BF16)
                dev0 = row0 // shard_rows
                qkv[grp, pl.ds(dev0, 2)] = val.reshape(2, n_seq, pos, val.shape[1])
            row_blocks(n_rows, 2 * shard_rows, body)

        def attend():
            def one_seq(seq, carry):
                length = lengths[grp * n_seq + seq]
                for head in range(n_heads):
                    prob = softmax_probs(seq_rows(qkv, grp, seq, head), seq_rows(qkv, grp, seq, n_heads + head), length, scale)
                    val = dot_nn(prob.astype(BF16), seq_rows(qkv, grp, seq, 2 * n_heads + head))
                    put_seq(ctx, grp, seq, head, val.astype(BF16))
                return carry
            lax.fori_loop(0, n_seq, one_seq, 0)
            save(qkv.at[grp], qkv_out.at[grp], 4 + grp)
            save(ctx.at[grp], ctx_out.at[grp], 6 + grp)
        return [project, attend]

    def part_dot(grp, row0, rows, col0, tile):
        lhs = ctx[grp, pl.ds(row0 // shard_rows, rows // shard_rows)].reshape(rows, n_heads * LANES)
        w_cols = w_out_v[:, :, pl.ds(pl.multiple_of(col0, tile), tile)].reshape(n_heads * LANES, tile)
        return dot_nn(lhs, w_cols)

    run_schedule(ring, stages, part_dot, on_full)
    for copy in saves:
        copy.wait()


def attn_bwd_kernel(n_dev, n_heads, scale, src, lengths, w_in, w_out, qkv_hbm, ctx_hbm, a_hbm, m_hbm, dpre_hbm,
                    out, g_in, g_out, g_up, full, act, qkv, dctx, dqkv, w_in_v, w_out_v, stage, stage_sem,
                     pbuf, precv, r_far, r_near, send_sem, recv_sem, own_sem, local_sem):
    ring = Ring(n_dev, src, full, pbuf, precv, r_far, r_near, out, send_sem, recv_sem, own_sem)
    ring.barrier()
    stager = Stager(stage, stage_sem.at[0])
    load_m = pltpu.make_async_copy(m_hbm, act, local_sem.at[2])
    load_dpre = pltpu.make_async_copy(dpre_hbm, dqkv, local_sem.at[3])
    load_dpre.start()
    load_m.start()
    load_out = load_heads(w_out, w_out_v, local_sem.at[1], True)
    load_qkv = pltpu.make_async_copy(qkv_hbm, qkv, local_sem.at[6])
    load_ctx = pltpu.make_async_copy(ctx_hbm, dctx, local_sem.at[4])
    load_qkv.start()
    load_in = load_heads(w_in, w_in_v, local_sem.at[0], True)
    load_a = pltpu.make_async_copy(a_hbm, act, local_sem.at[5])
    n_seq, pos = qkv.shape[2], qkv.shape[3]
    n_rows, d_model = full.shape[1], full.shape[2]
    shard_rows = n_seq * pos
    tile = n_heads * LANES
    head_dim = w_out.shape[1]

    def on_full(grp):
        if grp == 0:
            load_in.wait()
            load_out.wait()
            load_qkv.wait()
            load_a.start()

    def stages(grp):
        def project():
            def body(row0):
                w_all = w_out_v[...].reshape(n_heads * LANES, d_model)
                val = dot_nt(full[grp, pl.ds(row0, 2 * shard_rows), :], w_all).astype(BF16)
                dctx[grp, pl.ds(row0 // shard_rows, 2)] = val.reshape(2, n_seq, pos, val.shape[1])
            row_blocks(n_rows, 2 * shard_rows, body)

        def attend():
            def one_seq(seq, carry):
                length = lengths[grp * n_seq + seq]
                for head in range(n_heads):
                    q_val, k_val = seq_rows(qkv, grp, seq, head), seq_rows(qkv, grp, seq, n_heads + head)
                    v_val, dc_val = seq_rows(qkv, grp, seq, 2 * n_heads + head), seq_rows(dctx, grp, seq, head)
                    prob = softmax_probs(q_val, k_val, length, scale)
                    d_prob = dot_nt(dc_val, v_val).astype(BF16).astype(F32)
                    d_score = prob * (d_prob - jnp.sum(d_prob * prob, axis=1, keepdims=True))
                    d_score = (d_score * scale).astype(BF16)
                    put_seq(dqkv, grp, seq, head, dot_nn(d_score, k_val).astype(BF16))
                    put_seq(dqkv, grp, seq, n_heads + head, dot_tn(d_score, q_val).astype(BF16))
                    put_seq(dqkv, grp, seq, 2 * n_heads + head, dot_tn(prob.astype(BF16), dc_val).astype(BF16))
                return carry
            lax.fori_loop(0, n_seq, one_seq, 0)
            if grp + 1 == GROUPS:
                load_ctx.start()
        return [project, attend]

    def part_dot(grp, row0, rows, col0, width):
        n_cols = dqkv.shape[4]
        lhs = dqkv[grp, pl.ds(row0 // shard_rows, rows // shard_rows)].reshape(rows, n_cols)
        w_cols = w_in_v[:, :, pl.ds(pl.multiple_of(col0, width), width)].reshape(n_cols, width)
        return dot_nn(lhs, w_cols)

    def up_tile(step):
        def run():
            if step == 0:
                load_dpre.wait()
                load_m.wait()
            cols = pl.ds(step * tile, tile)
            n_cols = dqkv.shape[4]
            stager.put([lambda: dot_tn(act[:, :, cols].reshape(GROUPS * n_rows, tile), dqkv[...].reshape(GROUPS * n_rows, n_cols))], lambda ref: ref.at[:, :, pl.ds(0, n_cols)], g_up.at[pl.ds(step * n_heads, n_heads)])
        return run

    half = d_model // 2
    halves = (slice(0, half), slice(half, d_model))

    def heads_view(ref):
        return ref.at[:, pl.ds(0, head_dim), :]

    def out_grad():
        load_ctx.wait()
        stager.put([lambda lanes=lanes: dot_tn(dctx[...].reshape(GROUPS * n_rows, tile), full[:, :, lanes].reshape(GROUPS * n_rows, half))
                    for lanes in halves], heads_view, g_out)

    def in_tile(kind):
        def run():
            if kind == 0:
                load_a.wait()
            cols = pl.ds(kind * tile, tile)
            stager.put([lambda lanes=lanes: dot_tn(dqkv[:, :, :, :, cols].reshape(GROUPS * n_rows, tile), act[:, :, lanes].reshape(GROUPS * n_rows, half))
                        for lanes in halves], heads_view, g_in.at[pl.ds(kind * n_heads, n_heads)])
        return run

    n_up = d_model // tile
    ups = [up_tile(step) for step in range(n_up)]
    head = (ups[:n_up // 3], ups[n_up // 3:2 * (n_up // 3)], ups[2 * (n_up // 3):])
    run_schedule(ring, stages, part_dot, on_full, head, ([out_grad], [in_tile(0)], [in_tile(1), in_tile(2)]))
    stager.drain()


def gelu_tanh(pre_act):
    return jax.nn.gelu(pre_act, approximate=True)


def mlp_fwd_kernel(n_dev, src, w_up, b_up, w_down, out, full_out, pre_out,
                   full, pre, act, w_up_v, w_down_v, pbuf, precv, r_far, r_near, send_sem, recv_sem, own_sem, local_sem):
    ring = Ring(n_dev, src, full, pbuf, precv, r_far, r_near, out, send_sem, recv_sem, own_sem)
    ring.barrier()
    load_in = pltpu.make_async_copy(w_up, w_up_v, local_sem.at[0])
    load_out = pltpu.make_async_copy(w_down, w_down_v, local_sem.at[1])
    load_in.start()
    load_out.start()
    saves = []
    n_rows = full.shape[1]
    block = 2 * ring.rows

    def save(src_ref, dst_ref, idx):
        copy = pltpu.make_async_copy(src_ref, dst_ref, local_sem.at[idx])
        copy.start()
        saves.append(copy)

    def on_full(grp):
        if grp == 0:
            load_in.wait()
            load_out.wait()
        save(full.at[grp], full_out.at[grp], 2 + grp)

    def stages(grp):
        def project():
            def body(row0):
                rows = pl.ds(row0, block)
                val = dot_nn(full[grp, rows, :], w_up_v[...]) + b_up[...]
                pre[grp, rows, :] = val
                act[grp, rows, :] = gelu_tanh(val).astype(BF16)
            row_blocks(n_rows, block, body)
            save(pre.at[grp], pre_out.at[grp], 4 + grp)
        return [project]

    def part_dot(grp, row0, rows, col0, tile):
        return dot_nn(act[grp, pl.ds(row0, rows), :], w_down_v[:, pl.ds(pl.multiple_of(col0, tile), tile)])

    run_schedule(ring, stages, part_dot, on_full)
    for copy in saves:
        copy.wait()


def gelu_tanh_and_grad(pre_act, grad):
    coef = 0.7978845608028654
    square = pre_act * pre_act
    tanh_val = jnp.tanh(coef * (pre_act + 0.044715 * (square * pre_act)))
    cdf = 0.5 * (1.0 + tanh_val)
    slope = coef * (1.0 + 3.0 * 0.044715 * square)
    return pre_act * cdf, grad * (cdf + 0.5 * pre_act * (1.0 - tanh_val * tanh_val) * slope)


def mlp_bwd_kernel(n_dev, src, w_up, w_down, pre_hbm, out, dpre_out, dbias_out, g_down,
                   full, pre, act, dpre, w_up_v, w_down_v, stage, stage_sem,
                   pbuf, precv, r_far, r_near, send_sem, recv_sem, own_sem, local_sem):
    ring = Ring(n_dev, src, full, pbuf, precv, r_far, r_near, out, send_sem, recv_sem, own_sem)
    ring.barrier()
    stager = Stager(stage, stage_sem.at[0])
    load_in = pltpu.make_async_copy(w_up, w_up_v, local_sem.at[0])
    load_out = pltpu.make_async_copy(w_down, w_down_v, local_sem.at[1])
    load_pre = [pltpu.make_async_copy(pre_hbm.at[grp], pre, local_sem.at[2 + grp]) for grp in range(GROUPS)]
    for copy in (load_out, load_pre[0], load_in):
        copy.start()
    dbias_out[...] = jnp.zeros_like(dbias_out)
    saves = []
    n_rows = full.shape[1]
    block = 2 * ring.rows
    tile = act.shape[2] // 3

    def on_full(grp):
        if grp == 0:
            load_in.wait()
            load_out.wait()
        load_pre[grp].wait()

    def stages(grp):
        def project():
            def body(row0):
                rows = pl.ds(row0, block)
                d_act = dot_nt(full[grp, rows, :], w_down_v[...]).astype(BF16).astype(F32)
                act_val, d_pre = gelu_tanh_and_grad(pre[rows, :], d_act)
                act[grp, rows, :] = act_val.astype(BF16)
                dbias_out[...] += jnp.sum(d_pre, axis=0, keepdims=True)
                dpre[grp, rows, :] = d_pre.astype(BF16)
            row_blocks(n_rows, block, body)
            if grp + 1 < GROUPS:
                load_pre[grp + 1].start()
            copy = pltpu.make_async_copy(dpre.at[grp], dpre_out.at[grp], local_sem.at[4 + grp])
            copy.start()
            saves.append(copy)
        return [project]

    def part_dot(grp, row0, rows, col0, width):
        return dot_nt(dpre[grp, pl.ds(row0, rows), :], w_up_v[pl.ds(pl.multiple_of(col0, width), width), :])

    def down_tile(step):
        def run():
            cols = pl.ds(step * tile, tile)
            half = full.shape[2] // 2
            stager.put([lambda lanes=lanes: dot_tn(act[:, :, cols].reshape(GROUPS * n_rows, tile), full[:, :, lanes].reshape(GROUPS * n_rows, half))
                        for lanes in (slice(0, half), slice(half, 2 * half))], lambda ref: ref, g_down.at[cols, :])
        return run

    run_schedule(ring, stages, part_dot, on_full, tail=([down_tile(0)], [down_tile(1)], [down_tile(2)]))
    stager.drain()
    for copy in saves:
        copy.wait()


def ring_scratch(n_dev, rows, d_model):
    return [pltpu.VMEM((GROUPS, 4, 2, rows, d_model), BF16), pltpu.VMEM((GROUPS, 4, rows, d_model), BF16),
            pltpu.VMEM((GROUPS, 2, rows // 2, d_model), BF16), pltpu.VMEM((GROUPS, 2, rows, d_model), BF16),
            pltpu.SemaphoreType.DMA((GROUPS, N_COPIES)), pltpu.SemaphoreType.DMA((GROUPS, N_COPIES)),
            pltpu.SemaphoreType.DMA((GROUPS,)), pltpu.SemaphoreType.DMA((8,))]


def call_kernel(kernel, name, collective_id, out_shape, out_specs, in_specs, scratch, flops, args):
    return pl.pallas_call(
        kernel, out_shape=out_shape, in_specs=in_specs, out_specs=out_specs, scratch_shapes=scratch, name=name,
        cost_estimate=pl.CostEstimate(flops=flops, bytes_accessed=40_000_000, transcendentals=0),
        compiler_params=pltpu.CompilerParams(collective_id=collective_id, has_side_effects=True, vmem_limit_bytes=VMEM_LIMIT))(*args)


def shape(dims, dtype):
    return jax.ShapeDtypeStruct(dims, dtype)


def dims_of(shard, n_dev):
    n_seq, pos, d_model = shard.shape[0] // GROUPS, shard.shape[1], shard.shape[2]
    return n_seq, pos, n_seq * pos, n_dev * n_seq * pos, d_model


def attn_fwd(shard, lengths, w_in, w_out, n_dev, collective_id):
    n_seq, pos, rows, n_rows, d_model = dims_of(shard, n_dev)
    n_heads, head_dim = w_out.shape[0], w_out.shape[1]
    n_cols, c_cols = w_in.shape[0] * LANES, n_heads * LANES
    qkv_dims, ctx_dims = (GROUPS, n_dev, n_seq, pos, n_cols), (GROUPS, n_dev, n_seq, pos, c_cols)
    out, full, qkv, ctx = call_kernel(
        functools.partial(attn_fwd_kernel, n_dev, n_heads, head_dim ** -0.5), 'attn_fwd', collective_id,
        (shape((GROUPS, rows, d_model), BF16), shape((GROUPS, n_rows, d_model), BF16), shape(qkv_dims, BF16), shape(ctx_dims, BF16)),
        (VMEM, ANY, ANY, ANY), (VMEM, SMEM, ANY, ANY),
        [pltpu.VMEM((GROUPS, n_rows, d_model), BF16), pltpu.VMEM(qkv_dims, BF16), pltpu.VMEM(ctx_dims, BF16),
         pltpu.VMEM((w_in.shape[0], LANES, d_model), BF16), pltpu.VMEM((n_heads, LANES, d_model), BF16)] + ring_scratch(n_dev, rows, d_model),
        2 * GROUPS * n_rows * d_model * (n_cols + c_cols), (shard.reshape(GROUPS, rows, d_model), lengths, w_in, w_out))
    return out.reshape(shard.shape), full, qkv, ctx


def attn_bwd(shard, lengths, w_in, w_out, qkv, ctx, a_full, m_full, dpre, n_dev, collective_id):
    n_seq, pos, rows, n_rows, d_model = dims_of(shard, n_dev)
    n_heads, head_dim = w_out.shape[0], w_out.shape[1]
    n_cols, c_cols, ff = w_in.shape[0] * LANES, n_heads * LANES, dpre.shape[2]
    return call_kernel(
        functools.partial(attn_bwd_kernel, n_dev, n_heads, head_dim ** -0.5), 'attn_bwd', collective_id,
        (shape((GROUPS, rows, d_model), BF16), shape(w_in.shape, BF16), shape(w_out.shape, BF16), shape((d_model // LANES, LANES, ff), BF16)),
        (VMEM, ANY, ANY, ANY), (VMEM, SMEM) + (ANY,) * 7,
        [pltpu.VMEM((GROUPS, n_rows, d_model), BF16), pltpu.VMEM((GROUPS, n_rows, d_model), BF16),
         pltpu.VMEM(qkv.shape, BF16), pltpu.VMEM(ctx.shape, BF16), pltpu.VMEM(qkv.shape, BF16),
         pltpu.VMEM((w_in.shape[0], LANES, d_model), BF16), pltpu.VMEM((n_heads, LANES, d_model), BF16),
         pltpu.VMEM((2, n_heads, LANES, d_model), BF16), pltpu.SemaphoreType.DMA((1, 2))] + ring_scratch(n_dev, rows, d_model),
        4 * GROUPS * n_rows * d_model * (n_cols + c_cols), (shard.reshape(GROUPS, rows, d_model), lengths, w_in, w_out, qkv, ctx, a_full, m_full, dpre.reshape(qkv.shape)))


def mlp_fwd(shard, w_up, b_up, w_down, n_dev, collective_id):
    n_seq, pos, rows, n_rows, d_model = dims_of(shard, n_dev)
    ff = w_up.shape[1]
    out, full, pre = call_kernel(
        functools.partial(mlp_fwd_kernel, n_dev), 'mlp_fwd', collective_id,
        (shape((GROUPS, rows, d_model), BF16), shape((GROUPS, n_rows, d_model), BF16), shape((GROUPS, n_rows, ff), F32)),
        (VMEM, ANY, ANY), (VMEM, ANY, VMEM, ANY),
        [pltpu.VMEM((GROUPS, n_rows, d_model), BF16), pltpu.VMEM((GROUPS, n_rows, ff), F32), pltpu.VMEM((GROUPS, n_rows, ff), BF16),
         pltpu.VMEM(w_up.shape, BF16), pltpu.VMEM(w_down.shape, BF16)] + ring_scratch(n_dev, rows, d_model),
        4 * GROUPS * n_rows * d_model * ff, (shard.reshape(GROUPS, rows, d_model), w_up, b_up.reshape(1, ff), w_down))
    return out.reshape(shard.shape), full, pre


def mlp_bwd(shard, w_up, w_down, pre, n_dev, collective_id):
    n_seq, pos, rows, n_rows, d_model = dims_of(shard, n_dev)
    ff = w_up.shape[1]
    return call_kernel(
        functools.partial(mlp_bwd_kernel, n_dev), 'mlp_bwd', collective_id,
        (shape((GROUPS, rows, d_model), BF16), shape((GROUPS, n_rows, ff), BF16), shape((1, ff), F32), shape(w_down.shape, BF16)),
        (VMEM, ANY, VMEM, ANY), (VMEM, ANY, ANY, ANY),
        [pltpu.VMEM((GROUPS, n_rows, d_model), BF16), pltpu.VMEM((n_rows, ff), F32), pltpu.VMEM((GROUPS, n_rows, ff), BF16), pltpu.VMEM((GROUPS, n_rows, ff), BF16),
         pltpu.VMEM(w_up.shape, BF16), pltpu.VMEM(w_down.shape, BF16), pltpu.VMEM((2, ff // 3, d_model), BF16), pltpu.SemaphoreType.DMA((1, 2))] + ring_scratch(n_dev, rows, d_model),
        6 * GROUPS * n_rows * d_model * ff, (shard.reshape(GROUPS, rows, d_model), w_up, w_down, pre))


def sum_kernel(n_dev, parts, out, landed, total, send_sem, recv_sem):
    me = lax.axis_index(TENSOR_AXIS)
    others = [(me + step) % n_dev for step in range(1, n_dev)]
    sem = pltpu.get_barrier_semaphore()
    for dev in others:
        pl.semaphore_signal(sem, inc=1, device_id={TENSOR_AXIS: dev}, device_id_type=MESH)
    pl.semaphore_wait(sem, n_dev - 1)

    def copy(phase, idx, src_ref, dst_ref, dev):
        return pltpu.make_async_remote_copy(src_ref=src_ref, dst_ref=dst_ref, send_sem=send_sem.at[phase, idx], recv_sem=recv_sem.at[phase, idx],
                                            device_id={TENSOR_AXIS: dev}, device_id_type=MESH)
    sent = [copy(0, idx, parts.at[dev], landed.at[idx], dev) for idx, dev in enumerate(others)]
    for desc in sent:
        desc.start()
    acc = parts[me]
    for idx in range(n_dev - 1):
        sent[idx].wait_recv()
        acc = acc + landed[idx]
    total[...] = acc
    out[me] = acc
    spread = [copy(1, idx, total, out.at[me], dev) for idx, dev in enumerate(others)]
    for desc in spread:
        desc.start()
    for idx in range(n_dev - 1):
        origin = (me + n_dev - 1 - idx) % n_dev
        copy(1, idx, total, out.at[origin], origin).wait_recv()
    for desc in sent + spread:
        desc.wait_send()


def sum_over_devices(val, n_dev, collective_id):
    size = val.size
    per_dev = -(-size // (n_dev * LANES)) * LANES
    flat = jnp.pad(val.reshape(-1), (0, per_dev * n_dev - size)).reshape(n_dev, per_dev // LANES, LANES)
    out = pl.pallas_call(
        functools.partial(sum_kernel, n_dev), out_shape=shape(flat.shape, F32), in_specs=[VMEM], out_specs=VMEM, name='sum_devices',
        scratch_shapes=[pltpu.VMEM((n_dev - 1,) + flat.shape[1:], F32), pltpu.VMEM(flat.shape[1:], F32),
                        pltpu.SemaphoreType.DMA((2, n_dev - 1)), pltpu.SemaphoreType.DMA((2, n_dev - 1))],
        compiler_params=pltpu.CompilerParams(collective_id=collective_id, has_side_effects=True))(flat)
    return out.reshape(-1)[:size].reshape(val.shape)


def layer_norm(x_val, gain_vec, shift_vec):
    row_mean = jnp.mean(x_val, axis=-1, keepdims=True)
    centered = x_val - row_mean
    row_var = jnp.mean(centered * centered, axis=-1, keepdims=True)
    return centered * lax.rsqrt(row_var + 1e-5) * gain_vec + shift_vec


def layer_fwd(x_cur, lengths, weights, vec_layer, n_dev, collective_id):
    w_in, w_out, w_up, b_up, w_down = weights
    a_shard = layer_norm(x_cur, vec_layer[0], vec_layer[1]).astype(BF16)
    attn_shard, a_full, qkv, ctx = attn_fwd(a_shard, lengths, w_in, w_out, n_dev, collective_id)
    hidden = x_cur + attn_shard.astype(F32) + vec_layer[4]
    m_shard = layer_norm(hidden, vec_layer[2], vec_layer[3]).astype(BF16)
    mlp_shard, m_full, pre = mlp_fwd(m_shard, w_up, b_up, w_down, n_dev, collective_id + 1)
    x_next = hidden + mlp_shard.astype(F32) + vec_layer[5]
    return x_next, (x_cur, a_full, qkv, ctx, hidden, m_full, pre)


def layer_bwd(d_cur, residues, lengths, weights, vec_layer, n_dev, collective_id):
    w_in, w_out, w_up, _, w_down = weights
    x_prev, a_full, qkv, ctx, hidden, m_full, pre = residues
    n_heads, head_dim, d_model = w_out.shape
    d_mid, d_pre, g_bup, g_down = mlp_bwd(d_cur.astype(BF16), w_up, w_down, pre, n_dev, collective_id)
    d_hid_ln, d_gain2, d_shift2 = jax.vjp(layer_norm, hidden, vec_layer[2], vec_layer[3])[1](d_mid.reshape(d_cur.shape).astype(F32))
    d_hid = d_cur + d_hid_ln
    d_in, g_in, g_out, g_up = attn_bwd(d_hid.astype(BF16), lengths, w_in, w_out, qkv, ctx, a_full, m_full, d_pre, n_dev, collective_id + 1)
    d_x_ln, d_gain1, d_shift1 = jax.vjp(layer_norm, x_prev, vec_layer[0], vec_layer[1])[1](d_in.reshape(d_cur.shape).astype(F32))
    g_vec = jnp.stack([d_gain1, d_shift1, d_gain2, d_shift2, jnp.sum(d_hid, axis=(0, 1)), jnp.sum(d_cur, axis=(0, 1))])
    return d_hid + d_x_ln, (g_in, g_out, g_up.reshape(w_up.shape), g_bup[0], g_down, g_vec)


def group_body(n_dev, x_loc, dy_loc, len_loc, wqkv_loc, wout_loc, wup_loc, bup_loc, wdown_loc, vec_loc):
    n_layers, d_model, n_kinds, n_heads, head_dim = wqkv_loc.shape
    w_in_all = jnp.transpose(wqkv_loc, (0, 2, 3, 4, 1)).reshape(n_layers, n_kinds * n_heads, head_dim, d_model)
    saved_acts = []
    x_cur = x_loc
    weights_of = lambda idx: (w_in_all[idx], wout_loc[idx], wup_loc[idx], bup_loc[idx], wdown_loc[idx])
    for layer_idx in range(n_layers):
        x_cur, residues = layer_fwd(x_cur, len_loc, weights_of(layer_idx), vec_loc[layer_idx], n_dev, 2 * layer_idx)
        saved_acts.append(residues)
    d_cur = dy_loc.astype(F32)
    layer_grads = [None] * n_layers
    for layer_idx in reversed(range(n_layers)):
        d_cur, grad_set = layer_bwd(d_cur, saved_acts[layer_idx], len_loc, weights_of(layer_idx), vec_loc[layer_idx], n_dev,
                                    2 * n_layers + 2 * layer_idx)
        layer_grads[layer_idx] = grad_set
    stacked = [jnp.stack([grad_set[grad_pos] for grad_set in layer_grads]) for grad_pos in range(6)]
    g_vec = sum_over_devices(stacked[5], n_dev, 4 * n_layers)
    g_qkv = jnp.transpose(stacked[0].reshape(n_layers, n_kinds, n_heads, head_dim, d_model), (0, 4, 1, 2, 3))
    return x_cur, d_cur, g_qkv, stacked[1], stacked[2], stacked[3], stacked[4], g_vec


def solution(mesh):
    act_spec = P(PARTS_AXIS, TENSOR_AXIS, None)
    in_specs = (act_spec, act_spec, P(PARTS_AXIS), P(None, None, None, TENSOR_AXIS, None), P(None, TENSOR_AXIS, None, None), P(None, None, TENSOR_AXIS), P(None, TENSOR_AXIS), P(None, TENSOR_AXIS, None), P())
    out_specs = (act_spec, act_spec, P(PARTS_AXIS, None, None, TENSOR_AXIS, None), P(PARTS_AXIS, TENSOR_AXIS, None, None), P(PARTS_AXIS, None, TENSOR_AXIS), P(PARTS_AXIS, TENSOR_AXIS), P(PARTS_AXIS, TENSOR_AXIS, None), P(PARTS_AXIS, None, None))
    return jax.shard_map(functools.partial(group_body, mesh.shape[TENSOR_AXIS]), mesh=mesh, in_specs=in_specs, out_specs=out_specs, check_vma=False)
```

```python
import functools
import jax
import jax.numpy as jnp
from jax import lax
from jax.experimental import pallas as pl
from jax.experimental.pallas import tpu as pltpu
from jax.sharding import PartitionSpec as P

TENSOR_AXIS = 'tp'
PARTS_AXIS = 'dp'
MESH = pl.DeviceIdType.MESH
F32 = jnp.float32
BF16 = jnp.bfloat16
GROUPS = 2
LANES = 128
N_COPIES = 23
VMEM_LIMIT = 67043328
ANY = pl.BlockSpec(memory_space=pl.ANY)
VMEM = pl.BlockSpec(memory_space=pltpu.VMEM)
SMEM = pl.BlockSpec(memory_space=pltpu.SMEM)


def dot_nn(lhs, rhs):
    return lax.dot_general(lhs, rhs, (((1,), (0,)), ((), ())), preferred_element_type=F32)


def dot_nt(lhs, rhs):
    return lax.dot_general(lhs, rhs, (((1,), (1,)), ((), ())), preferred_element_type=F32)


def dot_tn(lhs, rhs):
    return lax.dot_general(lhs, rhs, (((0,), (0,)), ((), ())), preferred_element_type=F32)


class Ring:
    def __init__(self, n_dev, src, full, pbuf, precv, r_far, r_near, out, send_sem, recv_sem, own_sem):
        self.src, self.full, self.pbuf, self.precv = src, full, pbuf, precv
        self.r_far, self.r_near, self.out = r_far, r_near, out
        self.send_sem, self.recv_sem, self.own_sem = send_sem, recv_sem, own_sem
        self.rows = src.shape[1]
        self.half = self.rows // 2
        n_chips = n_dev // 2
        me = lax.axis_index(TENSOR_AXIS)
        chip, core = me // 2, me % 2
        self.me, self.core = me, core
        self.right_chip, self.left_chip = (chip + 1) % n_chips, (chip + n_chips - 1) % n_chips
        self.far_chip = (chip + 2) % n_chips
        self.chips = (self.far_chip, self.right_chip, self.left_chip, chip)
        self.partner = chip * 2 + 1 - core
        self.right, self.left, self.far = self.right_chip * 2 + core, self.left_chip * 2 + core, self.far_chip * 2 + core
        self.sent = {}

    def barrier(self):
        sem = pltpu.get_barrier_semaphore()
        for dev in (self.partner, self.left, self.right):
            pl.semaphore_signal(sem, inc=1, device_id={TENSOR_AXIS: dev}, device_id_type=MESH)
        pl.semaphore_wait(sem, 3)

    def copy(self, grp, idx, src, dst, dev):
        return pltpu.make_async_remote_copy(src_ref=src, dst_ref=dst, send_sem=self.send_sem.at[grp, idx],
                                            recv_sem=self.recv_sem.at[grp, idx], device_id={TENSOR_AXIS: dev}, device_id_type=MESH)

    def start(self, grp, idx, src, dst, dev):
        desc = self.copy(grp, idx, src, dst, dev)
        desc.start()
        self.sent[grp, idx] = desc

    def arrive(self, grp, idx, dst, dev):
        self.copy(grp, idx, dst, dst, dev).wait_recv()

    def slot(self, grp, shard, part=None):
        if part is None:
            return self.full.at[grp, pl.ds(pl.multiple_of(shard * self.rows, self.rows), self.rows), :]
        return self.full.at[grp, pl.ds(pl.multiple_of(shard * self.rows + part * self.half, self.half), self.half), :]

    def src_half(self, grp, part):
        return self.src.at[grp, pl.ds(part * self.half, self.half), :]

    def issue_own(self, grp):
        pltpu.make_async_copy(self.src.at[grp], self.slot(grp, self.me), self.own_sem.at[grp]).start()
        self.start(grp, 1, self.src_half(grp, 0), self.slot(grp, self.me, 0), self.right)
        self.start(grp, 3, self.src_half(grp, 1), self.slot(grp, self.me, 1), self.left)
        self.start(grp, 2, self.src_half(grp, 1), self.slot(grp, self.me, 1), self.right)
        self.start(grp, 4, self.src_half(grp, 0), self.slot(grp, self.me, 0), self.left)
        self.start(grp, 0, self.src.at[grp], self.slot(grp, self.me), self.partner)

    def pass_on(self, grp, idx, idx_next, idx_side, shard, part, dev_from, dev_to):
        here = self.slot(grp, shard, part)
        self.arrive(grp, idx, here, dev_from)
        if idx_next is not None:
            self.start(grp, idx_next, here, here, dev_to)
        self.start(grp, idx_side, here, here, self.partner)

    def serve_first(self, grp):
        self.pass_on(grp, 1, 5, 7, self.left, 0, self.left, self.right)
        self.pass_on(grp, 3, 6, 9, self.right, 1, self.right, self.left)

    def serve_second(self, grp):
        self.pass_on(grp, 2, None, 8, self.left, 1, self.left, None)
        self.pass_on(grp, 4, None, 10, self.right, 0, self.right, None)

    def serve_far(self, grp):
        self.pass_on(grp, 5, None, 11, self.far, 0, self.left, None)
        self.pass_on(grp, 6, None, 12, self.far, 1, self.right, None)

    def wait_full(self, grp):
        pltpu.make_async_copy(self.src.at[grp], self.slot(grp, self.me), self.own_sem.at[grp]).wait()
        other = 1 - self.core
        left, right, far = self.left_chip * 2 + other, self.right_chip * 2 + other, self.far_chip * 2 + other
        self.arrive(grp, 0, self.slot(grp, self.partner), self.partner)
        for idx, shard, part in ((7, left, 0), (9, right, 1), (8, left, 1), (10, right, 0), (11, far, 0), (12, far, 1)):
            self.arrive(grp, idx, self.slot(grp, shard, part), self.partner)

    def send_part(self, grp, k):
        self.start(grp, 13 + k, self.pbuf.at[k, 1 - self.core], self.precv.at[grp, k], self.partner)

    def sum_part(self, grp, k):
        mine = self.precv.at[grp, k]
        self.arrive(grp, 13 + k, mine, self.partner)
        total = self.pbuf[k, self.core].astype(F32) + mine[...].astype(F32)
        mine[...] = total.astype(BF16)
        first, second = mine.at[pl.ds(0, self.half), :], mine.at[pl.ds(self.half, self.half), :]
        if k == 0:
            self.start(grp, 17, first, self.r_far.at[grp, 0], self.right)
            self.start(grp, 18, second, self.r_far.at[grp, 1], self.left)
        elif k == 1:
            self.start(grp, 19, second, self.r_near.at[grp, 0, pl.ds(self.half, self.half), :], self.right)
        elif k == 2:
            self.start(grp, 20, first, self.r_near.at[grp, 1, pl.ds(0, self.half), :], self.left)

    def relay(self, grp):
        for k, side, part, idx_in, idx_out, dev_from, dev_to in (
                (1, 0, 0, 17, 21, self.left, self.right), (2, 1, 1, 18, 22, self.right, self.left)):
            landed = self.r_far.at[grp, side]
            self.arrive(grp, idx_in, landed, dev_from)
            part_rows = pl.ds(part * self.half, self.half)
            mine = self.precv.at[grp, k, part_rows, :]
            mine[...] = (mine[...].astype(F32) + landed[...].astype(F32)).astype(BF16)
            self.start(grp, idx_out, mine, self.r_near.at[grp, side, part_rows, :], dev_to)

    def finish(self, grp):
        low, high = pl.ds(0, self.half), pl.ds(self.half, self.half)
        self.arrive(grp, 19, self.r_near.at[grp, 0, high, :], self.left)
        self.arrive(grp, 20, self.r_near.at[grp, 1, low, :], self.right)
        self.arrive(grp, 21, self.r_near.at[grp, 0, low, :], self.left)
        self.arrive(grp, 22, self.r_near.at[grp, 1, high, :], self.right)
        total = self.precv[grp, 3].astype(F32) + self.r_near[grp, 0].astype(F32) + self.r_near[grp, 1].astype(F32)
        return total.astype(BF16).astype(F32)

    def settle(self, grp, idx):
        self.sent.pop((grp, idx)).wait_send()

    def drain(self):
        for desc in self.sent.values():
            desc.wait_send()


def run_schedule(ring, stages, part_dot, on_full, epilogue, head=((), (), ()), tail=((), (), ())):
    def fill(work):
        for fn in work:
            fn()

    def parts(grp, k):
        rows = ring.rows
        row0 = pl.multiple_of(ring.chips[k] * 2 * rows, 2 * rows)
        width = ring.out.shape[2]
        tile = width // 3

        def column(step, carry):
            cols = pl.ds(pl.multiple_of(step * tile, tile), tile)
            val = part_dot(grp, row0, 2 * rows, step * tile, tile).astype(BF16)
            ring.pbuf[k, 0, :, cols] = val[:rows]
            ring.pbuf[k, 1, :, cols] = val[rows:]
            return carry
        if grp > 0:
            ring.settle(grp - 1, 13 + k)
        lax.fori_loop(0, 3, column, 0)
        ring.send_part(grp, k)

    ring.issue_own(0)
    fill(head[0])
    ring.serve_first(0)
    ring.issue_own(1)
    fill(head[1])
    ring.serve_second(0)
    fill(head[2])
    ring.serve_far(0)
    ring.wait_full(0)
    on_full(0)
    stages_0 = stages(0)
    stages_0[0]()
    ring.serve_first(1)
    for fn in stages_0[1:]:
        fn()
    parts(0, 0)
    ring.serve_second(1)
    parts(0, 1)
    ring.sum_part(0, 0)
    parts(0, 2)
    ring.sum_part(0, 1)
    parts(0, 3)
    ring.sum_part(0, 2)
    ring.serve_far(1)
    ring.sum_part(0, 3)
    ring.wait_full(1)
    on_full(1)
    stages_1 = stages(1)
    stages_1[0]()
    ring.relay(0)
    for fn in stages_1[1:]:
        fn()
    parts(1, 0)
    parts(1, 1)
    ring.sum_part(1, 0)
    parts(1, 2)
    ring.sum_part(1, 1)
    parts(1, 3)
    ring.sum_part(1, 2)
    fill(tail[0])
    epilogue(0, ring.finish(0))
    ring.sum_part(1, 3)
    fill(tail[1])
    ring.relay(1)
    fill(tail[2])
    epilogue(1, ring.finish(1))
    ring.drain()


def add_norm(base_hbm, vecs, rows_of, hid_hbm, out, base, sem, saves):
    add_row, gain_row, shift_row = rows_of
    load = pltpu.make_async_copy(base_hbm, base, sem.at[8])
    load.start()

    def vec(row):
        return vecs[row[0], pl.ds(row[1], 1), :]

    def epilogue(grp, total):
        if grp == 0:
            load.wait()
        val = base[grp] + total + vec(add_row)
        base[grp] = val
        store = pltpu.make_async_copy(base.at[grp], hid_hbm.at[grp], sem.at[9 + grp])
        store.start()
        saves.append(store)
        out[grp] = layer_norm(val, vec(gain_row), vec(shift_row)).astype(BF16)
    return epilogue


class NormGrad:
    def __init__(self, base_hbm, dres_hbm, vecs, gain_row, new_hbm, out, vgrad, base, dres, new, sem):
        self.base_hbm, self.dres_hbm, self.new_hbm = base_hbm, dres_hbm, new_hbm
        self.vecs, self.gain_row, self.out, self.vgrad = vecs, gain_row, out, vgrad
        self.base, self.dres, self.new, self.sem = base, dres, new, sem
        self.store = None
        vgrad[...] = jnp.zeros_like(vgrad)
        self.load(0)

    def load(self, grp):
        self.loads = [pltpu.make_async_copy(self.base_hbm.at[grp], self.base, self.sem.at[0]),
                      pltpu.make_async_copy(self.dres_hbm.at[grp], self.dres, self.sem.at[1])]
        for copy in self.loads:
            copy.start()

    def __call__(self, grp, d_norm):
        for copy in self.loads:
            copy.wait()
        x_val, d_res = self.base[...], self.dres[...]
        centered = x_val - jnp.mean(x_val, axis=-1, keepdims=True)
        inv_std = lax.rsqrt(jnp.mean(centered * centered, axis=-1, keepdims=True) + 1e-5)
        x_hat = centered * inv_std
        d_hat = d_norm * self.vecs[self.gain_row[0], pl.ds(self.gain_row[1], 1), :]
        mean_d = jnp.mean(d_hat, axis=-1, keepdims=True)
        mean_dx = jnp.mean(d_hat * x_hat, axis=-1, keepdims=True)
        d_new = d_res + inv_std * (d_hat - mean_d - x_hat * mean_dx)
        for row, val in enumerate((d_norm * x_hat, d_norm, d_new, d_res)):
            self.vgrad[pl.ds(row, 1), :] += jnp.sum(val, axis=0, keepdims=True)
        if self.store is not None:
            self.store.wait()
        self.new[...] = d_new
        self.out[grp] = d_new.astype(BF16)
        self.store = pltpu.make_async_copy(self.new, self.new_hbm.at[grp], self.sem.at[2])
        self.store.start()
        if grp + 1 < GROUPS:
            self.load(grp + 1)

    def drain(self):
        self.store.wait()


def row_blocks(n_rows, block, body):
    def step(i, carry):
        body(pl.multiple_of(i * block, block))
        return carry
    lax.fori_loop(0, n_rows // block, step, 0)


class Stager:
    def __init__(self, buf, sem):
        self.buf, self.sem, self.pending, self.count = buf, sem, [None, None], 0

    def put(self, pieces, view, dst):
        slot = self.count % 2
        self.count += 1
        if self.pending[slot] is not None:
            self.pending[slot].wait()
        start = 0
        for piece in pieces:
            val = piece().astype(self.buf.dtype)
            lanes = pl.ds(start, val.shape[1])
            start += val.shape[1]
            if len(self.buf.shape) == 4:
                self.buf[slot, :, :, lanes] = val.reshape(self.buf.shape[1], self.buf.shape[2], val.shape[1])
            else:
                self.buf[slot, :, lanes] = val
        copy = pltpu.make_async_copy(view(self.buf.at[slot]), dst, self.sem.at[slot])
        copy.start()
        self.pending[slot] = copy

    def drain(self):
        for copy in self.pending:
            if copy is not None:
                copy.wait()


def load_heads(hbm, vmem, sem, pad):
    head_dim = hbm.shape[1]
    copy = pltpu.make_async_copy(hbm, vmem.at[:, pl.ds(0, head_dim), :], sem)
    copy.start()
    if pad:
        vmem[:, head_dim:, :] = jnp.zeros((vmem.shape[0], LANES - head_dim, vmem.shape[2]), vmem.dtype)
    return copy


def softmax_probs(q_val, k_val, length, scale):
    scores = dot_nt(q_val, k_val) * scale
    row = lax.broadcasted_iota(jnp.int32, scores.shape, 0)
    col = lax.broadcasted_iota(jnp.int32, scores.shape, 1)
    scores = jnp.where((col <= row) & (col < length), scores, -1e30)
    expd = jnp.exp(scores - jnp.max(scores, axis=1, keepdims=True))
    return expd / jnp.sum(expd, axis=1, keepdims=True)


def seq_rows(ref, grp, seq, head):
    block = ref[grp, :, seq, :, head * LANES:(head + 1) * LANES]
    return block.reshape(block.shape[0] * block.shape[1], LANES)


def put_seq(ref, grp, seq, head, val):
    n_dev, pos = ref.shape[1], ref.shape[3]
    ref[grp, :, seq, :, head * LANES:(head + 1) * LANES] = val.reshape(n_dev, pos, LANES)


def attn_fwd_kernel(n_dev, n_heads, scale, layer, rows_of, src, lengths, w_in, w_out, base, vecs, out, hid, full_out, qkv_out, ctx_out,
                    full, qkv, ctx, w_in_v, w_out_v, e_base, pbuf, precv, r_far, r_near, send_sem, recv_sem, own_sem, local_sem):
    ring = Ring(n_dev, src, full, pbuf, precv, r_far, r_near, out, send_sem, recv_sem, own_sem)
    ring.barrier()
    load_in = load_heads(w_in.at[layer], w_in_v, local_sem.at[0], True)
    load_out = load_heads(w_out.at[layer], w_out_v, local_sem.at[1], True)
    saves = []
    epilogue = add_norm(base, vecs, rows_of, hid, out, e_base, local_sem, saves)
    n_seq, pos = qkv.shape[2], qkv.shape[3]
    n_rows, d_model = full.shape[1], full.shape[2]
    shard_rows = n_seq * pos

    def save(src_ref, dst_ref, idx):
        copy = pltpu.make_async_copy(src_ref, dst_ref, local_sem.at[idx])
        copy.start()
        saves.append(copy)

    def on_full(grp):
        if grp == 0:
            load_in.wait()
            load_out.wait()
        save(full.at[grp], full_out.at[grp], 2 + grp)

    def stages(grp):
        def project():
            def body(row0):
                w_all = w_in_v[...].reshape(w_in_v.shape[0] * LANES, d_model)
                val = dot_nt(full[grp, pl.ds(row0, 2 * shard_rows), :], w_all).astype(BF16)
                dev0 = row0 // shard_rows
                qkv[grp, pl.ds(dev0, 2)] = val.reshape(2, n_seq, pos, val.shape[1])
            row_blocks(n_rows, 2 * shard_rows, body)

        def attend():
            def one_seq(seq, carry):
                length = lengths[grp * n_seq + seq]
                for head in range(n_heads):
                    prob = softmax_probs(seq_rows(qkv, grp, seq, head), seq_rows(qkv, grp, seq, n_heads + head), length, scale)
                    val = dot_nn(prob.astype(BF16), seq_rows(qkv, grp, seq, 2 * n_heads + head))
                    put_seq(ctx, grp, seq, head, val.astype(BF16))
                return carry
            lax.fori_loop(0, n_seq, one_seq, 0)
            save(qkv.at[grp], qkv_out.at[grp], 4 + grp)
            save(ctx.at[grp], ctx_out.at[grp], 6 + grp)
        return [project, attend]

    def part_dot(grp, row0, rows, col0, tile):
        lhs = ctx[grp, pl.ds(row0 // shard_rows, rows // shard_rows)].reshape(rows, n_heads * LANES)
        w_cols = w_out_v[:, :, pl.ds(pl.multiple_of(col0, tile), tile)].reshape(n_heads * LANES, tile)
        return dot_nn(lhs, w_cols)

    run_schedule(ring, stages, part_dot, on_full, epilogue)
    for copy in saves:
        copy.wait()


def attn_bwd_kernel(n_dev, n_heads, scale, layer, src, lengths, w_in, w_out, qkv_hbm, ctx_hbm, a_hbm, m_hbm, dpre_hbm, base_hbm, dres_hbm, vecs,
                    out, new_hbm, vgrad, g_in, g_out, g_up, full, act, qkv, dctx, dqkv, w_in_v, w_out_v, stage, stage_sem, e_base, e_dres, e_new, e_sem,
                     pbuf, precv, r_far, r_near, send_sem, recv_sem, own_sem, local_sem):
    ring = Ring(n_dev, src, full, pbuf, precv, r_far, r_near, out, send_sem, recv_sem, own_sem)
    ring.barrier()
    stager = Stager(stage, stage_sem.at[0])
    load_m = pltpu.make_async_copy(m_hbm, act, local_sem.at[2])
    load_dpre = pltpu.make_async_copy(dpre_hbm, dqkv, local_sem.at[3])
    load_dpre.start()
    load_m.start()
    load_qkv = pltpu.make_async_copy(qkv_hbm, qkv, local_sem.at[6])
    load_ctx = pltpu.make_async_copy(ctx_hbm, dctx, local_sem.at[4])
    late = []

    def late_loads():
        late.append(load_heads(w_out.at[layer], w_out_v, local_sem.at[1], True))
        load_qkv.start()
        late.append(load_qkv)
        late.append(load_heads(w_in.at[layer], w_in_v, local_sem.at[0], True))
    epilogue = NormGrad(base_hbm, dres_hbm, vecs, (layer, 0), new_hbm, out, vgrad, e_base, e_dres, e_new, e_sem)
    load_a = pltpu.make_async_copy(a_hbm, act, local_sem.at[5])
    n_seq, pos = qkv.shape[2], qkv.shape[3]
    n_rows, d_model = full.shape[1], full.shape[2]
    shard_rows = n_seq * pos
    tile = n_heads * LANES
    head_dim = w_out.shape[2]

    def on_full(grp):
        if grp == 0:
            for copy in late:
                copy.wait()
            load_a.start()

    def stages(grp):
        def project():
            def body(row0):
                w_all = w_out_v[...].reshape(n_heads * LANES, d_model)
                val = dot_nt(full[grp, pl.ds(row0, 2 * shard_rows), :], w_all).astype(BF16)
                dctx[grp, pl.ds(row0 // shard_rows, 2)] = val.reshape(2, n_seq, pos, val.shape[1])
            row_blocks(n_rows, 2 * shard_rows, body)

        def attend():
            def one_seq(seq, carry):
                length = lengths[grp * n_seq + seq]
                for head in range(n_heads):
                    q_val, k_val = seq_rows(qkv, grp, seq, head), seq_rows(qkv, grp, seq, n_heads + head)
                    v_val, dc_val = seq_rows(qkv, grp, seq, 2 * n_heads + head), seq_rows(dctx, grp, seq, head)
                    prob = softmax_probs(q_val, k_val, length, scale)
                    d_prob = dot_nt(dc_val, v_val).astype(BF16).astype(F32)
                    d_score = prob * (d_prob - jnp.sum(d_prob * prob, axis=1, keepdims=True))
                    d_score = (d_score * scale).astype(BF16)
                    put_seq(dqkv, grp, seq, head, dot_nn(d_score, k_val).astype(BF16))
                    put_seq(dqkv, grp, seq, n_heads + head, dot_tn(d_score, q_val).astype(BF16))
                    put_seq(dqkv, grp, seq, 2 * n_heads + head, dot_tn(prob.astype(BF16), dc_val).astype(BF16))
                return carry
            lax.fori_loop(0, n_seq, one_seq, 0)
            if grp + 1 == GROUPS:
                load_ctx.start()
        return [project, attend]

    def part_dot(grp, row0, rows, col0, width):
        n_cols = dqkv.shape[4]
        lhs = dqkv[grp, pl.ds(row0 // shard_rows, rows // shard_rows)].reshape(rows, n_cols)
        w_cols = w_in_v[:, :, pl.ds(pl.multiple_of(col0, width), width)].reshape(n_cols, width)
        return dot_nn(lhs, w_cols)

    def up_tile(step):
        def run():
            if step == 0:
                load_dpre.wait()
                load_m.wait()
            cols = pl.ds(step * tile, tile)
            n_cols = dqkv.shape[4]
            stager.put([lambda: dot_tn(act[:, :, cols].reshape(GROUPS * n_rows, tile), dqkv[...].reshape(GROUPS * n_rows, n_cols))], lambda ref: ref.at[:, :, pl.ds(0, n_cols)], g_up.at[pl.ds(step * n_heads, n_heads)])
        return run

    half = d_model // 2
    halves = (slice(0, half), slice(half, d_model))

    def heads_view(ref):
        return ref.at[:, pl.ds(0, head_dim), :]

    def out_grad():
        load_ctx.wait()
        stager.put([lambda lanes=lanes: dot_tn(dctx[...].reshape(GROUPS * n_rows, tile), full[:, :, lanes].reshape(GROUPS * n_rows, half))
                    for lanes in halves], heads_view, g_out)

    def in_tile(kind):
        def run():
            if kind == 0:
                load_a.wait()
            cols = pl.ds(kind * tile, tile)
            stager.put([lambda lanes=lanes: dot_tn(dqkv[:, :, :, :, cols].reshape(GROUPS * n_rows, tile), act[:, :, lanes].reshape(GROUPS * n_rows, half))
                        for lanes in halves], heads_view, g_in.at[pl.ds(kind * n_heads, n_heads)])
        return run

    n_up = d_model // tile
    ups = [up_tile(step) for step in range(n_up)]
    head = ([], [late_loads] + ups[:n_up // 2], ups[n_up // 2:])
    run_schedule(ring, stages, part_dot, on_full, epilogue, head, ([out_grad], [in_tile(0)], [in_tile(1), in_tile(2)]))
    stager.drain()
    epilogue.drain()


def gelu_tanh(pre_act):
    return jax.nn.gelu(pre_act, approximate=True)


def mlp_fwd_kernel(n_dev, layer, rows_of, src, w_up, b_up, w_down, base, vecs, out, hid, full_out, pre_out,
                   full, pre, act, w_up_v, w_down_v, e_base, pbuf, precv, r_far, r_near, send_sem, recv_sem, own_sem, local_sem):
    ring = Ring(n_dev, src, full, pbuf, precv, r_far, r_near, out, send_sem, recv_sem, own_sem)
    ring.barrier()
    load_in = pltpu.make_async_copy(w_up.at[layer], w_up_v, local_sem.at[0])
    load_out = pltpu.make_async_copy(w_down.at[layer], w_down_v, local_sem.at[1])
    load_in.start()
    load_out.start()
    saves = []
    epilogue = add_norm(base, vecs, rows_of, hid, out, e_base, local_sem, saves)
    n_rows = full.shape[1]
    block = 2 * ring.rows

    def save(src_ref, dst_ref, idx):
        copy = pltpu.make_async_copy(src_ref, dst_ref, local_sem.at[idx])
        copy.start()
        saves.append(copy)

    def on_full(grp):
        if grp == 0:
            load_in.wait()
            load_out.wait()
        save(full.at[grp], full_out.at[grp], 2 + grp)

    def stages(grp):
        def project():
            def body(row0):
                rows = pl.ds(row0, block)
                val = dot_nn(full[grp, rows, :], w_up_v[...]) + b_up[...]
                pre[grp, rows, :] = val
                act[grp, rows, :] = gelu_tanh(val).astype(BF16)
            row_blocks(n_rows, block, body)
            save(pre.at[grp], pre_out.at[grp], 4 + grp)
        return [project]

    def part_dot(grp, row0, rows, col0, tile):
        return dot_nn(act[grp, pl.ds(row0, rows), :], w_down_v[:, pl.ds(pl.multiple_of(col0, tile), tile)])

    run_schedule(ring, stages, part_dot, on_full, epilogue)
    for copy in saves:
        copy.wait()


def gelu_tanh_and_grad(pre_act, grad):
    coef = 0.7978845608028654
    square = pre_act * pre_act
    tanh_val = jnp.tanh(coef * (pre_act + 0.044715 * (square * pre_act)))
    cdf = 0.5 * (1.0 + tanh_val)
    slope = coef * (1.0 + 3.0 * 0.044715 * square)
    return pre_act * cdf, grad * (cdf + 0.5 * pre_act * (1.0 - tanh_val * tanh_val) * slope)


def mlp_bwd_kernel(n_dev, layer, src, w_up, w_down, pre_hbm, base_hbm, dres_hbm, vecs, out, new_hbm, vgrad, dpre_out, dbias_out, g_down,
                   full, pre, act, dpre, w_up_v, w_down_v, stage, stage_sem, e_base, e_dres, e_new, e_sem,
                   pbuf, precv, r_far, r_near, send_sem, recv_sem, own_sem, local_sem):
    ring = Ring(n_dev, src, full, pbuf, precv, r_far, r_near, out, send_sem, recv_sem, own_sem)
    ring.barrier()
    stager = Stager(stage, stage_sem.at[0])
    load_in = pltpu.make_async_copy(w_up.at[layer], w_up_v, local_sem.at[0])
    load_out = pltpu.make_async_copy(w_down.at[layer], w_down_v, local_sem.at[1])
    load_pre = [pltpu.make_async_copy(pre_hbm.at[grp], pre, local_sem.at[2 + grp]) for grp in range(GROUPS)]
    for copy in (load_out, load_pre[0], load_in):
        copy.start()
    epilogue = NormGrad(base_hbm, dres_hbm, vecs, (layer, 2), new_hbm, out, vgrad, e_base, e_dres, e_new, e_sem)
    dbias_out[...] = jnp.zeros_like(dbias_out)
    saves = []
    n_rows = full.shape[1]
    block = 2 * ring.rows
    tile = act.shape[2] // 3

    def on_full(grp):
        if grp == 0:
            load_in.wait()
            load_out.wait()
        load_pre[grp].wait()

    def stages(grp):
        def project():
            def body(row0):
                rows = pl.ds(row0, block)
                d_act = dot_nt(full[grp, rows, :], w_down_v[...]).astype(BF16).astype(F32)
                act_val, d_pre = gelu_tanh_and_grad(pre[rows, :], d_act)
                act[grp, rows, :] = act_val.astype(BF16)
                dbias_out[...] += jnp.sum(d_pre, axis=0, keepdims=True)
                dpre[grp, rows, :] = d_pre.astype(BF16)
            row_blocks(n_rows, block, body)
            if grp + 1 < GROUPS:
                load_pre[grp + 1].start()
            copy = pltpu.make_async_copy(dpre.at[grp], dpre_out.at[grp], local_sem.at[4 + grp])
            copy.start()
            saves.append(copy)
        return [project]

    def part_dot(grp, row0, rows, col0, width):
        return dot_nt(dpre[grp, pl.ds(row0, rows), :], w_up_v[pl.ds(pl.multiple_of(col0, width), width), :])

    def down_tile(step):
        def run():
            cols = pl.ds(step * tile, tile)
            half = full.shape[2] // 2
            stager.put([lambda lanes=lanes: dot_tn(act[:, :, cols].reshape(GROUPS * n_rows, tile), full[:, :, lanes].reshape(GROUPS * n_rows, half))
                        for lanes in (slice(0, half), slice(half, 2 * half))], lambda ref: ref, g_down.at[cols, :])
        return run

    run_schedule(ring, stages, part_dot, on_full, epilogue, tail=([down_tile(0)], [down_tile(1)], [down_tile(2)]))
    stager.drain()
    epilogue.drain()
    for copy in saves:
        copy.wait()


def ring_scratch(n_dev, rows, d_model):
    return [pltpu.VMEM((4, 2, rows, d_model), BF16), pltpu.VMEM((GROUPS, 4, rows, d_model), BF16),
            pltpu.VMEM((GROUPS, 2, rows // 2, d_model), BF16), pltpu.VMEM((GROUPS, 2, rows, d_model), BF16),
            pltpu.SemaphoreType.DMA((GROUPS, N_COPIES)), pltpu.SemaphoreType.DMA((GROUPS, N_COPIES)),
            pltpu.SemaphoreType.DMA((GROUPS,)), pltpu.SemaphoreType.DMA((12,))]


def call_kernel(kernel, name, collective_id, out_shape, out_specs, in_specs, scratch, flops, args):
    return pl.pallas_call(
        kernel, out_shape=out_shape, in_specs=in_specs, out_specs=out_specs, scratch_shapes=scratch, name=name,
        cost_estimate=pl.CostEstimate(flops=flops, bytes_accessed=40_000_000, transcendentals=0),
        compiler_params=pltpu.CompilerParams(collective_id=collective_id, has_side_effects=True, vmem_limit_bytes=VMEM_LIMIT))(*args)


def shape(dims, dtype):
    return jax.ShapeDtypeStruct(dims, dtype)


def dims_of(shard, seq_pos, n_dev):
    rows, d_model = shard.shape[1], shard.shape[2]
    return rows // seq_pos, seq_pos, rows, n_dev * rows, d_model


def attn_fwd(layer, rows_of, shard, base, vecs, pos, lengths, w_in, w_out, n_dev, collective_id):
    n_seq, pos, rows, n_rows, d_model = dims_of(shard, pos, n_dev)
    n_heads, head_dim = w_out.shape[1], w_out.shape[2]
    n_cols, c_cols = w_in.shape[1] * LANES, n_heads * LANES
    qkv_dims, ctx_dims = (GROUPS, n_dev, n_seq, pos, n_cols), (GROUPS, n_dev, n_seq, pos, c_cols)
    return call_kernel(
        functools.partial(attn_fwd_kernel, n_dev, n_heads, head_dim ** -0.5, layer, rows_of), 'attn_fwd', collective_id,
        (shape(shard.shape, BF16), shape(shard.shape, F32), shape((GROUPS, n_rows, d_model), BF16), shape(qkv_dims, BF16), shape(ctx_dims, BF16)),
        (VMEM, ANY, ANY, ANY, ANY), (VMEM, SMEM, ANY, ANY, ANY, VMEM),
        [pltpu.VMEM((GROUPS, n_rows, d_model), BF16), pltpu.VMEM(qkv_dims, BF16), pltpu.VMEM(ctx_dims, BF16),
         pltpu.VMEM((w_in.shape[1], LANES, d_model), BF16), pltpu.VMEM((n_heads, LANES, d_model), BF16), pltpu.VMEM(base.shape, F32)] + ring_scratch(n_dev, rows, d_model),
        2 * GROUPS * n_rows * d_model * (n_cols + c_cols), (shard, lengths, w_in, w_out, base, vecs))


def mlp_fwd(layer, rows_of, shard, base, vecs, pos, w_up, b_up, w_down, n_dev, collective_id):
    n_seq, pos, rows, n_rows, d_model = dims_of(shard, pos, n_dev)
    ff = w_up.shape[2]
    return call_kernel(
        functools.partial(mlp_fwd_kernel, n_dev, layer, rows_of), 'mlp_fwd', collective_id,
        (shape(shard.shape, BF16), shape(shard.shape, F32), shape((GROUPS, n_rows, d_model), BF16), shape((GROUPS, n_rows, ff), F32)),
        (VMEM, ANY, ANY, ANY), (VMEM, ANY, VMEM, ANY, ANY, VMEM),
        [pltpu.VMEM((GROUPS, n_rows, d_model), BF16), pltpu.VMEM((GROUPS, n_rows, ff), F32), pltpu.VMEM((GROUPS, n_rows, ff), BF16),
         pltpu.VMEM(w_up.shape[1:], BF16), pltpu.VMEM(w_down.shape[1:], BF16), pltpu.VMEM(base.shape, F32)] + ring_scratch(n_dev, rows, d_model),
        4 * GROUPS * n_rows * d_model * ff, (shard, w_up, b_up[layer].reshape(1, ff), w_down, base, vecs))


def norm_grad_scratch(rows, d_model):
    return [pltpu.VMEM((rows, d_model), F32)] * 3 + [pltpu.SemaphoreType.DMA((3,))]


def attn_bwd(layer, shard, base, d_res, vecs, pos, lengths, w_in, w_out, qkv, ctx, a_full, m_full, dpre, n_dev, collective_id):
    n_seq, pos, rows, n_rows, d_model = dims_of(shard, pos, n_dev)
    n_heads, head_dim = w_out.shape[1], w_out.shape[2]
    n_cols, c_cols, ff = w_in.shape[1] * LANES, n_heads * LANES, dpre.shape[2]
    return call_kernel(
        functools.partial(attn_bwd_kernel, n_dev, n_heads, head_dim ** -0.5, layer), 'attn_bwd', collective_id,
        (shape(shard.shape, BF16), shape(shard.shape, F32), shape((4, d_model), F32),
         shape(w_in.shape[1:], BF16), shape(w_out.shape[1:], BF16), shape((d_model // LANES, LANES, ff), BF16)),
        (VMEM, ANY, VMEM, ANY, ANY, ANY), (VMEM, SMEM) + (ANY,) * 9 + (VMEM,),
        [pltpu.VMEM((GROUPS, n_rows, d_model), BF16), pltpu.VMEM((GROUPS, n_rows, d_model), BF16),
         pltpu.VMEM(qkv.shape, BF16), pltpu.VMEM(ctx.shape, BF16), pltpu.VMEM(qkv.shape, BF16),
         pltpu.VMEM((w_in.shape[1], LANES, d_model), BF16), pltpu.VMEM((n_heads, LANES, d_model), BF16),
         pltpu.VMEM((2, n_heads, LANES, d_model), BF16), pltpu.SemaphoreType.DMA((1, 2))] + norm_grad_scratch(rows, d_model) + ring_scratch(n_dev, rows, d_model),
        4 * GROUPS * n_rows * d_model * (n_cols + c_cols),
        (shard, lengths, w_in, w_out, qkv, ctx, a_full, m_full, dpre.reshape(qkv.shape), base, d_res, vecs))


def mlp_bwd(layer, shard, base, d_res, vecs, pos, w_up, w_down, pre, n_dev, collective_id):
    n_seq, pos, rows, n_rows, d_model = dims_of(shard, pos, n_dev)
    ff = w_up.shape[2]
    return call_kernel(
        functools.partial(mlp_bwd_kernel, n_dev, layer), 'mlp_bwd', collective_id,
        (shape(shard.shape, BF16), shape(shard.shape, F32), shape((4, d_model), F32),
         shape((GROUPS, n_rows, ff), BF16), shape((1, ff), F32), shape(w_down.shape[1:], BF16)),
        (VMEM, ANY, VMEM, ANY, VMEM, ANY), (VMEM,) + (ANY,) * 5 + (VMEM,),
        [pltpu.VMEM((GROUPS, n_rows, d_model), BF16), pltpu.VMEM((n_rows, ff), F32), pltpu.VMEM((GROUPS, n_rows, ff), BF16), pltpu.VMEM((GROUPS, n_rows, ff), BF16),
         pltpu.VMEM(w_up.shape[1:], BF16), pltpu.VMEM(w_down.shape[1:], BF16), pltpu.VMEM((2, ff // 3, d_model), BF16),
         pltpu.SemaphoreType.DMA((1, 2))] + norm_grad_scratch(rows, d_model) + ring_scratch(n_dev, rows, d_model),
        6 * GROUPS * n_rows * d_model * ff, (shard, w_up, w_down, pre, base, d_res, vecs))


def stack_kernel(n_layers, n_arrays, *refs):
    n_in = n_layers * n_arrays
    ins, outs, bufs = refs[:n_in], refs[n_in:n_in + n_arrays], refs[n_in + n_arrays:n_in + 2 * n_arrays]
    load_sem, store_sem = refs[n_in + 2 * n_arrays:]
    pairs = [(pos, layer) for pos in range(n_arrays) for layer in range(n_layers)]
    loads = [pltpu.make_async_copy(ins[layer * n_arrays + pos], bufs[pos].at[layer], load_sem.at[idx]) for idx, (pos, layer) in enumerate(pairs)]
    stores = [pltpu.make_async_copy(bufs[pos].at[layer], outs[pos].at[layer], store_sem.at[idx]) for idx, (pos, layer) in enumerate(pairs)]
    for copy in loads:
        copy.start()
    for load, store in zip(loads, stores):
        load.wait()
        store.start()
    for copy in stores:
        copy.wait()


def stack_layers(layer_arrays):
    n_layers, n_arrays = len(layer_arrays), len(layer_arrays[0])
    shapes = [(n_layers,) + val.shape for val in layer_arrays[0]]
    flat = [val for arrays in layer_arrays for val in arrays]
    return pl.pallas_call(
        functools.partial(stack_kernel, n_layers, n_arrays), out_shape=tuple(shape(dims, BF16) for dims in shapes),
        in_specs=[ANY] * len(flat), out_specs=(ANY,) * n_arrays, name='stack_layers',
        scratch_shapes=[pltpu.VMEM(dims, BF16) for dims in shapes] + [pltpu.SemaphoreType.DMA((len(flat),)), pltpu.SemaphoreType.DMA((len(flat),))],
        cost_estimate=pl.CostEstimate(flops=0, bytes_accessed=100_000_000, transcendentals=0),
        compiler_params=pltpu.CompilerParams(vmem_limit_bytes=VMEM_LIMIT))(*flat)


def sum_kernel(n_dev, parts, out, landed, total, send_sem, recv_sem):
    me = lax.axis_index(TENSOR_AXIS)
    others = [(me + step) % n_dev for step in range(1, n_dev)]
    sem = pltpu.get_barrier_semaphore()
    for dev in others:
        pl.semaphore_signal(sem, inc=1, device_id={TENSOR_AXIS: dev}, device_id_type=MESH)
    pl.semaphore_wait(sem, n_dev - 1)

    def copy(phase, idx, src_ref, dst_ref, dev):
        return pltpu.make_async_remote_copy(src_ref=src_ref, dst_ref=dst_ref, send_sem=send_sem.at[phase, idx], recv_sem=recv_sem.at[phase, idx],
                                            device_id={TENSOR_AXIS: dev}, device_id_type=MESH)
    sent = [copy(0, idx, parts.at[dev], landed.at[idx], dev) for idx, dev in enumerate(others)]
    for desc in sent:
        desc.start()
    acc = parts[me]
    for idx in range(n_dev - 1):
        sent[idx].wait_recv()
        acc = acc + landed[idx]
    total[...] = acc
    out[me] = acc
    spread = [copy(1, idx, total, out.at[me], dev) for idx, dev in enumerate(others)]
    for desc in spread:
        desc.start()
    for idx in range(n_dev - 1):
        origin = (me + n_dev - 1 - idx) % n_dev
        copy(1, idx, total, out.at[origin], origin).wait_recv()
    for desc in sent + spread:
        desc.wait_send()


def sum_over_devices(val, n_dev, collective_id):
    size = val.size
    per_dev = -(-size // (n_dev * LANES)) * LANES
    flat = jnp.pad(val.reshape(-1), (0, per_dev * n_dev - size)).reshape(n_dev, per_dev // LANES, LANES)
    out = pl.pallas_call(
        functools.partial(sum_kernel, n_dev), out_shape=shape(flat.shape, F32), in_specs=[VMEM], out_specs=VMEM, name='sum_devices',
        scratch_shapes=[pltpu.VMEM((n_dev - 1,) + flat.shape[1:], F32), pltpu.VMEM(flat.shape[1:], F32),
                        pltpu.SemaphoreType.DMA((2, n_dev - 1)), pltpu.SemaphoreType.DMA((2, n_dev - 1))],
        compiler_params=pltpu.CompilerParams(collective_id=collective_id, has_side_effects=True))(flat)
    return out.reshape(-1)[:size].reshape(val.shape)


def layer_norm(x_val, gain_vec, shift_vec):
    row_mean = jnp.mean(x_val, axis=-1, keepdims=True)
    centered = x_val - row_mean
    row_var = jnp.mean(centered * centered, axis=-1, keepdims=True)
    return centered * lax.rsqrt(row_var + 1e-5) * gain_vec + shift_vec


def group_body(n_dev, x_loc, dy_loc, len_loc, wqkv_loc, wout_loc, wup_loc, bup_loc, wdown_loc, vec_loc):
    n_layers, d_model, n_kinds, n_heads, head_dim = wqkv_loc.shape
    w_in_all = jnp.transpose(wqkv_loc, (0, 2, 3, 4, 1)).reshape(n_layers, n_kinds * n_heads, head_dim, d_model)
    pos = x_loc.shape[1]
    rows_shape = (GROUPS, x_loc.shape[0] // GROUPS * pos, d_model)
    x_cur = x_loc.reshape(rows_shape)
    shard = layer_norm(x_cur, vec_loc[0, 0], vec_loc[0, 1]).astype(BF16)
    saved = []
    for layer in range(n_layers):
        after = min(layer + 1, n_layers - 1)
        mid_shard, hidden, a_full, qkv, ctx = attn_fwd(layer, ((layer, 4), (layer, 2), (layer, 3)), shard, x_cur, vec_loc, pos, len_loc,
                                                       w_in_all, wout_loc, n_dev, 2 * layer)
        shard, x_next, m_full, pre = mlp_fwd(layer, ((layer, 5), (after, 0), (after, 1)), mid_shard, hidden, vec_loc, pos,
                                             wup_loc, bup_loc, wdown_loc, n_dev, 2 * layer + 1)
        saved.append((x_cur, a_full, qkv, ctx, hidden, m_full, pre))
        x_cur = x_next
    shard = dy_loc.reshape(rows_shape)
    d_cur = shard.astype(F32)
    layer_grads, small_grads = [None] * n_layers, [None] * n_layers
    for layer in reversed(range(n_layers)):
        x_prev, a_full, qkv, ctx, hidden, m_full, pre = saved[layer]
        first_id = 2 * n_layers + 2 * layer
        mid_shard, d_hid, v_mlp, d_pre, g_bup, g_down = mlp_bwd(layer, shard, hidden, d_cur, vec_loc, pos, wup_loc, wdown_loc, pre, n_dev, first_id)
        shard, d_cur, v_attn, g_in, g_out, g_up = attn_bwd(layer, mid_shard, x_prev, d_hid, vec_loc, pos, len_loc, w_in_all, wout_loc,
                                                           qkv, ctx, a_full, m_full, d_pre, n_dev, first_id + 1)
        layer_grads[layer] = (g_in, g_out, g_up.reshape(wup_loc.shape[1:]), g_down)
        small_grads[layer] = (g_bup[0], jnp.concatenate([v_attn[:2], v_mlp]))
    g_vec = sum_over_devices(jnp.stack([grad_set[1] for grad_set in small_grads]), n_dev, 4 * n_layers)
    g_bup = jnp.stack([grad_set[0] for grad_set in small_grads])
    g_in, g_out, g_up, g_down = stack_layers(layer_grads)
    g_qkv = jnp.transpose(g_in.reshape(n_layers, n_kinds, n_heads, head_dim, d_model), (0, 4, 1, 2, 3))
    return x_cur.reshape(x_loc.shape), d_cur.reshape(x_loc.shape), g_qkv, g_out, g_up, g_bup, g_down, g_vec


def solution(mesh):
    act_spec = P(PARTS_AXIS, TENSOR_AXIS, None)
    in_specs = (act_spec, act_spec, P(PARTS_AXIS), P(None, None, None, TENSOR_AXIS, None), P(None, TENSOR_AXIS, None, None), P(None, None, TENSOR_AXIS), P(None, TENSOR_AXIS), P(None, TENSOR_AXIS, None), P())
    out_specs = (act_spec, act_spec, P(PARTS_AXIS, None, None, TENSOR_AXIS, None), P(PARTS_AXIS, TENSOR_AXIS, None, None), P(PARTS_AXIS, None, TENSOR_AXIS), P(PARTS_AXIS, TENSOR_AXIS), P(PARTS_AXIS, TENSOR_AXIS, None), P(PARTS_AXIS, None, None))
    return jax.shard_map(functools.partial(group_body, mesh.shape[TENSOR_AXIS]), mesh=mesh, in_specs=in_specs, out_specs=out_specs, check_vma=False)
```
